32 devices in a mesh: din: 4 (over x, core), dout: 8 (over z, y).
Axes of the slice: x: 2, y: 2, z: 4, core: 2. Of those that a mesh axis runs over, the one named last changes fastest.
Arguments:
- inputs: float32 [16, 8192], P('dout', 'din'), may hold values from -1.5 to 1.5
- out_grad: float32 [16, 28672], P('din', 'dout'), may hold values from -6 to 6
- weight: float32 [8192, 28672], P('din', 'dout'), may hold values from -0.03125 to 0.03125
Outputs:
- input_grad: float32 [16, 8192], P('dout', 'din')
- weight_grad: float32 [8192, 28672], P('din', 'dout')
The draws below stay inside these ranges and needn't reach their ends.
All inputs are finite; a program needn't handle non-finite values.
Results may differ from the reference program's by a relative error of at most 0.000071.
Values sent between devices are 32-bit elements; how exact they have to be, the bound alone decides.
No kernel may reach another device: no remote copies, remote signals or barrier semaphores. Data moves between devices by JAX's collectives and lax.ppermute only.
A program may use at most 128 MiB of HBM per device.

```python
import jax
import jax.numpy as jnp
from jax import lax

D = 8192
FF = 28672
ROWS = 16


def with_spikes(values, stream_key, source, target, blocks, factor):
    owner, partner = [(jnp.arange(values.shape[axis_at]) // (values.shape[axis_at] // blocks)).reshape([-1 if axis == axis_at else 1 for axis in range(values.ndim)]) for axis_at in (source, target)]
    chosen = jax.random.permutation(stream_key, blocks)[partner]
    strong = (owner == chosen) | (owner == (partner + blocks // 2) % blocks)
    return jnp.where(strong, factor * values, values)


def shard_levels(key, extent, pieces, smallest, top_value):
    def one(position, blocks):
        heights = jax.random.uniform(jax.random.fold_in(jax.random.fold_in(key, 6), position), (blocks,), jnp.float32, smallest / len(pieces), top_value / len(pieces))
        return jnp.repeat(jnp.exp(heights), extent[position] // blocks).reshape((-1,) + (1,) * (len(extent) - position - 1))

    gain = one(*pieces[0])
    for cut in pieces[1:]:
        gain = gain * one(*cut)
    return gain


def gaussian(stream_key, extent, width, reach, pieces=(), kind=jnp.bfloat16):
    entries = width * jax.random.normal(stream_key, extent, jnp.float32)
    if pieces:
        entries = entries * shard_levels(stream_key, extent, pieces, -0.22, 0.18)
    return jnp.clip(entries, -reach, reach).astype(kind)


def heavy_noise(key, shape, spread, reach, cuts, heavy, held_as=jnp.bfloat16):
    values = spread * jax.random.normal(key, shape, jnp.float32)
    if cuts:
        values = values * shard_levels(key, shape, cuts, -0.22, 0.18)
    return jnp.clip(with_spikes(values, jax.random.fold_in(key, 3), *heavy), -reach, reach).astype(held_as)


def setup_inputs(seed: int = 0) -> dict:
    key_list = jax.random.split(jax.random.key(seed), 4)
    inputs = gaussian(key_list[0], (ROWS, D), (ROWS ** -0.5), 1.5, ((0, 8), (1, 4)), jnp.float32)
    out_grad = heavy_noise(key_list[1], (ROWS, FF), 1.0, 6.0, ((0, 4), (1, 8)), (1, 0, 8, 2.0), jnp.float32)
    weight = gaussian(key_list[2], (D, FF), FF ** -0.5, 0.03125, ((0, 4), (1, 8)), jnp.float32)
    return {"inputs": inputs, "out_grad": out_grad, "weight": weight}


def reference(inputs, out_grad, weight):
    weight_grad = lax.dot_general(inputs, out_grad, (((0,), (0,)), ((), ())), precision=lax.Precision.HIGHEST, preferred_element_type=jnp.float32)
    input_grad = lax.dot_general(out_grad, weight, (((1,), (1,)), ((), ())), precision=lax.Precision.HIGHEST, preferred_element_type=jnp.float32)
    return input_grad, weight_grad
```

```python
import functools

import jax
import jax.numpy as jnp
from jax import lax
from jax.experimental import pallas as pl
from jax.experimental.pallas import tpu as pltpu
from jax.sharding import PartitionSpec as P

F32 = jnp.float32
BF16 = jnp.bfloat16
TN = (((0,), (0,)), ((), ()))
NT = (((1,), (1,)), ((), ()))


def plain_body(inputs, out_grad, weight):
    gradients = lax.all_gather(out_grad, "din", axis=0, tiled=True)
    rows = lax.all_gather(inputs, "dout", axis=0, tiled=True)
    weight_grad = lax.dot_general(
        rows, gradients, TN, precision=lax.Precision.HIGHEST, preferred_element_type=F32
    )
    partial = lax.dot_general(
        gradients, weight, NT, precision=lax.Precision.HIGHEST, preferred_element_type=F32
    )
    input_grad = lax.psum_scatter(partial, "dout", scatter_dimension=0, tiled=True)
    return (input_grad, weight_grad)


def halves(value):
    high = value.astype(BF16)
    low = (value - high.astype(F32)).astype(BF16)
    return high, low


def swap(value, axis, size, distance):
    return lax.ppermute(value, axis, [(i, i ^ distance) for i in range(size)])


def in_order(pieces, me):
    count = len(pieces)
    ordered = []
    for position in range(count):
        value = pieces[0][...]
        for s in range(1, count):
            value = jnp.where((me ^ s) == position, pieces[s][...], value)
        ordered.append(value)
    return ordered


def units_kernel(count, groups, *refs):
    grads, refs = refs[:count], refs[count:]
    w_ref, refs = refs[0], refs[1:]
    outs, (split_ref, rows_ref, stack_ref) = refs[:groups], refs[groups:]
    rows = rows_ref.shape[0]
    block = rows // count

    @pl.when(pl.program_id(0) == 0)
    def _():
        for position, value in enumerate(in_order(grads, lax.axis_index("din"))):
            rows_ref[position * block : (position + 1) * block, :] = value
        high, low = halves(rows_ref[...])
        split_ref[...] = jnp.concatenate([high, low, high], axis=0)

    high, low = halves(w_ref[...])
    both = lax.dot_general(split_ref[: 2 * rows], high, NT, preferred_element_type=F32)
    rest = lax.dot_general(split_ref[:rows], low, NT, preferred_element_type=F32)
    total = both[:rows] + both[rows:] + rest
    part = rows // groups
    for position in range(groups):
        stack_ref[position] = total[position * part : (position + 1) * part]
    me = lax.axis_index("dout") // 2
    for s in range(groups):
        outs[s][...] = stack_ref[me ^ s]


def units(grads, weight, groups, tile):
    depth, width = weight.shape
    count = len(grads)
    block = grads[0].shape[0]
    rows = count * block
    part = rows // groups
    return pl.pallas_call(
        functools.partial(units_kernel, count, groups),
        grid=(depth // tile,),
        out_shape=[jax.ShapeDtypeStruct((part, depth), F32)] * groups
        + [jax.ShapeDtypeStruct((3 * rows, width), BF16)],
        in_specs=[pl.BlockSpec((block, width), lambda i: (0, 0))] * count
        + [pl.BlockSpec((tile, width), lambda i: (i, 0))],
        out_specs=[pl.BlockSpec((part, tile), lambda i: (0, i))] * groups
        + [pl.BlockSpec((3 * rows, width), lambda i: (0, 0))],
        scratch_shapes=[
            pltpu.VMEM((rows, width), F32),
            pltpu.VMEM((groups, part, tile), F32),
        ],
        compiler_params=pltpu.CompilerParams(
            vmem_limit_bytes=48 << 20, dimension_semantics=("arbitrary",)
        ),
        name="units",
    )(*grads, weight)


def rows_kernel(count, with_buffer, *refs):
    pieces, refs = refs[:count], refs[count:]
    split_ref = refs[0]
    out_ref, rows_ref = refs[-2:]
    rows = rows_ref.shape[0]
    block = rows // count
    for position, value in enumerate(in_order(pieces, lax.axis_index("dout") // 2)):
        rows_ref[position * block : (position + 1) * block, :] = value
    high, low = halves(rows_ref[...])
    out_ref[...] = lax.dot_general(
        jnp.concatenate([high, high, low], axis=0),
        split_ref[...],
        TN,
        preferred_element_type=F32,
    )


def outer(pieces, split, buffer, first, steps, tile):
    count = len(pieces)
    block, depth = pieces[0].shape
    width = split.shape[1]
    operands = [*pieces, split] + ([buffer] if buffer is not None else [])
    return pl.pallas_call(
        functools.partial(rows_kernel, count, buffer is not None),
        grid=(steps,),
        out_shape=jax.ShapeDtypeStruct((depth, width), F32),
        in_specs=[pl.BlockSpec((block, tile), lambda i: (0, i + first))] * count
        + [pl.BlockSpec(split.shape, lambda i: (0, 0))]
        + ([pl.BlockSpec(memory_space=pl.ANY)] if buffer is not None else []),
        out_specs=pl.BlockSpec((tile, width), lambda i: (i + first, 0)),
        scratch_shapes=[pltpu.VMEM((count * block, tile), F32)],
        input_output_aliases={count + 1: 0} if buffer is not None else {},
        compiler_params=pltpu.CompilerParams(
            vmem_limit_bytes=40 << 20, dimension_semantics=("arbitrary",)
        ),
        name="outer_first" if buffer is None else "outer_rest",
    )(*operands)


def body(n_in, n_out, inputs, out_grad, weight):
    groups = n_out // 2
    tile = 256
    odd = lax.axis_index("dout") % 2 == 1
    near = swap(inputs, "dout", n_out, 1)
    grads = [out_grad] + [swap(out_grad, "din", n_in, s) for s in range(1, n_in)]
    pair = jnp.where(
        odd, jnp.concatenate([near, inputs], 0), jnp.concatenate([inputs, near], 0)
    )
    pieces = [pair] + [swap(pair, "dout", n_out, 2 * s) for s in range(1, groups)]
    *parts, split = units(grads, weight, groups, tile)
    steps = weight.shape[0] // tile
    moved = [parts[0]] + [
        swap(parts[s], "dout", n_out, 2 * s) for s in range(1, groups)
    ]
    first = outer(pieces, split, None, 0, steps // 2, tile)
    summed = sum(moved[1:], moved[0])
    half = summed.shape[0] // 2
    keep = jnp.where(odd, summed[half:], summed[:half])
    give = jnp.where(odd, summed[:half], summed[half:])
    taken = swap(give, "dout", n_out, 1)
    weight_grad = outer(pieces, split, first, steps // 2, steps - steps // 2, tile)
    return (keep + taken, weight_grad)


def power_of_two(value):
    return value & (value - 1) == 0


def solution(mesh):
    n_in, n_out = mesh.shape["din"], mesh.shape["dout"]

    def run(inputs, out_grad, weight):
        depth, width = weight.shape
        fits = (
            power_of_two(n_in)
            and power_of_two(n_out)
            and n_in <= 8
            and 4 <= n_out <= 8
            and inputs.shape[0] * n_out <= 64
            and depth % 512 == 0
            and width % 128 == 0
        )
        if not fits:
            return plain_body(inputs, out_grad, weight)
        return body(n_in, n_out, inputs, out_grad, weight)

    placed = (P("dout", "din"), P("din", "dout"), P("din", "dout"))
    return jax.shard_map(
        run,
        mesh=mesh,
        in_specs=placed,
        out_specs=(P("dout", "din"), P("din", "dout")),
        check_vma=False,
    )
```

```python
import functools

import jax
import jax.numpy as jnp
from jax import lax
from jax.experimental import pallas as pl
from jax.experimental.pallas import tpu as pltpu
from jax.sharding import PartitionSpec as P


F32 = jnp.float32
BF16 = jnp.bfloat16
TN = (((0,), (0,)), ((), ()))
NT = (((1,), (1,)), ((), ()))

UNITS_TILE = 256
BOTH_TILE = 128
OUTER_TILE = 128
READ_SLOTS = 4
WRITE_SLOTS = 3


def plain_body(inputs, out_grad, weight):
    gradients = lax.all_gather(out_grad, "din", axis=0, tiled=True)
    rows = lax.all_gather(inputs, "dout", axis=0, tiled=True)
    weight_grad = lax.dot_general(
        rows, gradients, TN, precision=lax.Precision.HIGHEST, preferred_element_type=F32
    )
    partial = lax.dot_general(
        gradients, weight, NT, precision=lax.Precision.HIGHEST, preferred_element_type=F32
    )
    input_grad = lax.psum_scatter(partial, "dout", scatter_dimension=0, tiled=True)
    return (input_grad, weight_grad)


def halves(value):
    high = value.astype(BF16)
    low = (value - high.astype(F32)).astype(BF16)
    return high, low


def swap(value, axis, size, distance):
    return lax.ppermute(value, axis, [(i, i ^ distance) for i in range(size)])


def in_order(pieces, me):
    count = len(pieces)
    ordered = []
    for position in range(count):
        value = pieces[0][...]
        for s in range(1, count):
            value = jnp.where((me ^ s) == position, pieces[s][...], value)
        ordered.append(value)
    return ordered


def multiply(split_ref, rows, value):
    high, low = halves(value)
    both = lax.dot_general(split_ref[: 2 * rows], high, NT, preferred_element_type=F32)
    rest = lax.dot_general(split_ref[:rows], low, NT, preferred_element_type=F32)
    return both[:rows] + both[rows:] + rest


def aligned(index, tile):
    return pl.ds(pl.multiple_of(index * tile, tile), tile)


class Reader:
    def __init__(self, w_ref, slots, sems, first, steps):
        self.w, self.slots, self.sems = w_ref, slots, sems
        self.first, self.steps = first, steps
        self.ahead = min(slots.shape[0] - 1, steps)

    def copy(self, step):
        count, tile = self.slots.shape[:2]
        slot = lax.rem(step, count)
        return pltpu.make_async_copy(
            self.w.at[aligned(self.first + step, tile), :],
            self.slots.at[slot],
            self.sems.at[slot],
        )

    def begin(self):
        for step in range(self.ahead):
            self.copy(step).start()

    def take(self, step):
        self.copy(step).wait()

        @pl.when(step + self.ahead < self.steps)
        def _():
            self.copy(step + self.ahead).start()

        return self.slots[lax.rem(step, self.slots.shape[0])]


class Writer:
    def __init__(self, left_ref, split_ref, out_ref, slots, sems, first, steps):
        self.left, self.split, self.out = left_ref, split_ref, out_ref
        self.slots, self.sems = slots, sems
        self.first, self.steps = first, steps

    def copy(self, step):
        count, tile = self.slots.shape[:2]
        slot = lax.rem(step, count)
        return pltpu.make_async_copy(
            self.slots.at[slot],
            self.out.at[aligned(self.first + step, tile), :],
            self.sems.at[slot],
        )

    def make(self, step):
        count, tile = self.slots.shape[:2]

        @pl.when(step >= count)
        def _():
            self.copy(step - count).wait()

        self.slots[lax.rem(step, count)] = lax.dot_general(
            self.left[:, aligned(self.first + step, tile)],
            self.split[...],
            TN,
            preferred_element_type=F32,
        )
        self.copy(step).start()

    def finish(self):
        for step in range(max(0, self.steps - self.slots.shape[0]), self.steps):
            self.copy(step).wait()


def loop(steps, run):
    def one(step, carry):
        run(step)
        return carry

    lax.fori_loop(0, steps, one, 0)


def units_kernel(count, steps, *refs):
    grads, refs = refs[:count], refs[count:]
    w_ref, out_ref, split_ref, rows_ref, slots, sems = refs
    reader = Reader(w_ref, slots, sems, 0, steps)
    reader.begin()
    rows = rows_ref.shape[0]
    block = rows // count
    for position, value in enumerate(in_order(grads, lax.axis_index("din"))):
        rows_ref[position * block : (position + 1) * block, :] = value
    high, low = halves(rows_ref[...])
    split_ref[...] = jnp.concatenate([high, low, high], axis=0)

    def run(step):
        tile = slots.shape[1]
        out_ref[:, aligned(step, tile)] = multiply(split_ref, rows, reader.take(step))

    loop(steps, run)


def in_vmem(count=1):
    return [pl.BlockSpec(memory_space=pltpu.VMEM)] * count


def in_hbm(count=1):
    return [pl.BlockSpec(memory_space=pltpu.MemorySpace.HBM)] * count


def ring(slots, tile, width):
    return [pltpu.VMEM((slots, tile, width), F32), pltpu.SemaphoreType.DMA((slots,))]


def units(grads, weight, steps, tile):
    width = weight.shape[1]
    count = len(grads)
    rows = sum(piece.shape[0] for piece in grads)
    return pl.pallas_call(
        functools.partial(units_kernel, count, steps),
        out_shape=[
            pltpu.VMEM((rows, steps * tile), F32),
            pltpu.VMEM((3 * rows, width), BF16),
        ],
        in_specs=in_vmem(count) + in_hbm(),
        out_specs=in_vmem(2),
        scratch_shapes=[pltpu.VMEM((rows, width), F32)] + ring(READ_SLOTS, tile, width),
        compiler_params=pltpu.CompilerParams(vmem_limit_bytes=28 << 20),
        name="units",
    )(*grads, weight)


def both_kernel(count, steps, *refs):
    pieces, refs = refs[:count], refs[count:]
    (
        split_ref, begun_ref, w_ref, total_ref, left_ref, out_ref, rows_ref,
        read_slots, read_sems, write_slots, write_sems,
    ) = refs
    tile = read_slots.shape[1]
    rows = rows_ref.shape[0]
    begun = begun_ref.shape[1]
    reader = Reader(w_ref, read_slots, read_sems, begun // tile, steps)
    reader.begin()
    block = rows // count
    for position, value in enumerate(in_order(pieces, lax.axis_index("dout") // 2)):
        rows_ref[position * block : (position + 1) * block, :] = value
    high, low = halves(rows_ref[...])
    left_ref[...] = jnp.concatenate([high, high, low], axis=0)
    writer = Writer(left_ref, split_ref, out_ref, write_slots, write_sems, 0, steps)

    def run(step):
        writer.make(step)
        total_ref[:, aligned(begun // tile + step, tile)] = multiply(
            split_ref, rows, reader.take(step)
        )

    loop(steps, run)
    total_ref[:, :begun] = begun_ref[...]
    writer.finish()


def both(pieces, split, begun, weight, tile):
    depth, width = weight.shape
    count = len(pieces)
    rows = begun.shape[0]
    steps = (depth - begun.shape[1]) // tile
    return pl.pallas_call(
        functools.partial(both_kernel, count, steps),
        out_shape=[
            pltpu.VMEM((rows, depth), F32),
            pltpu.VMEM((3 * rows, depth), BF16),
            jax.ShapeDtypeStruct((depth, width), F32),
        ],
        in_specs=in_vmem(count + 2) + in_hbm(),
        out_specs=in_vmem(2) + in_hbm(),
        scratch_shapes=[pltpu.VMEM((rows, depth), F32)]
        + ring(READ_SLOTS, tile, width)
        + ring(WRITE_SLOTS, tile, width),
        compiler_params=pltpu.CompilerParams(vmem_limit_bytes=32 << 20),
        name="both",
    )(*pieces, split, begun, weight)


def outer_kernel(first, steps, left_ref, split_ref, begun_ref, out_ref, slots, sems):
    del begun_ref
    writer = Writer(left_ref, split_ref, out_ref, slots, sems, first, steps)
    loop(steps, writer.make)
    writer.finish()


def outer(left, split, buffer, first, steps, tile):
    depth, width = left.shape[1], split.shape[1]
    return pl.pallas_call(
        functools.partial(outer_kernel, first, steps),
        out_shape=jax.ShapeDtypeStruct((depth, width), F32),
        in_specs=in_vmem(2) + in_hbm(),
        out_specs=in_hbm()[0],
        scratch_shapes=ring(min(steps, WRITE_SLOTS), tile, width),
        input_output_aliases={2: 0},
        compiler_params=pltpu.CompilerParams(vmem_limit_bytes=24 << 20),
    )(left, split, buffer)


def bit_of(axis, distance):
    return (lax.axis_index(axis) // distance) % 2 == 1


def joined(value, n_out, distance):
    other = swap(value, "dout", n_out, distance)
    return jnp.where(
        bit_of("dout", distance),
        jnp.concatenate([other, value], 0),
        jnp.concatenate([value, other], 0),
    )


def halved(value, n_out, distance):
    half = value.shape[0] // 2
    upper = bit_of("dout", distance)
    keep = jnp.where(upper, value[half:], value[:half])
    give = jnp.where(upper, value[:half], value[half:])
    return keep + swap(give, "dout", n_out, distance)


def body(n_in, n_out, inputs, out_grad, weight):
    depth = weight.shape[0]
    rounds = n_out.bit_length() - 1
    weight = pltpu.with_memory_space_constraint(weight, pltpu.MemorySpace.HBM)
    grads = [out_grad] + [swap(out_grad, "din", n_in, s) for s in range(1, n_in)]
    pair = joined(inputs, n_out, 1)
    pieces = [pair]
    pieces += [swap(pair, "dout", n_out, 2 * s) for s in range(1, n_out // 2)]
    begun, split = units(grads, weight, depth // UNITS_TILE // 2, UNITS_TILE)
    total, left, weight_grad = both(pieces, split, begun, weight, BOTH_TILE)
    parts = depth // OUTER_TILE
    first = parts // 2
    rest = parts - first
    for r in range(rounds):
        total = halved(total, n_out, n_out >> (r + 1))
        steps = (rest + rounds - 1 - r) // (rounds - r)
        rest -= steps
        weight_grad = outer(left, split, weight_grad, first, steps, OUTER_TILE)
        first += steps
    return (total, weight_grad)


def power_of_two(value):
    return value & (value - 1) == 0


def solution(mesh):
    n_in, n_out = mesh.shape["din"], mesh.shape["dout"]
    shaped = (
        power_of_two(n_in) and power_of_two(n_out) and n_in <= 8 and 4 <= n_out <= 8
    )

    def run(inputs, out_grad, weight):
        depth, width = weight.shape
        fits = (
            inputs.shape[0] * n_out <= 64
            and depth % (2 * UNITS_TILE) == 0
            and depth >= 8 * UNITS_TILE
            and width % 128 == 0
        )
        if not (shaped and fits):
            return plain_body(inputs, out_grad, weight)
        return body(n_in, n_out, inputs, out_grad, weight)

    placed = (P("dout", "din"), P("din", "dout"), P("din", "dout"))
    return jax.shard_map(
        run,
        mesh=mesh,
        in_specs=placed,
        out_specs=(P("dout", "din"), P("din", "dout")),
        check_vma=False,
    )
```

```python
import functools

import jax
import jax.numpy as jnp
from jax import lax
from jax.experimental import pallas as pl
from jax.experimental.pallas import tpu as pltpu
from jax.sharding import PartitionSpec as P


F32 = jnp.float32
BF16 = jnp.bfloat16
TN = (((0,), (0,)), ((), ()))
NT = (((1,), (1,)), ((), ()))

UNITS_TILE = 256
OUTER_TILE = 128
READ_SLOTS = 4
WRITE_SLOTS = 4
CUTS = 2


def plain_body(inputs, out_grad, weight):
    gradients = lax.all_gather(out_grad, "din", axis=0, tiled=True)
    rows = lax.all_gather(inputs, "dout", axis=0, tiled=True)
    weight_grad = lax.dot_general(
        rows, gradients, TN, precision=lax.Precision.HIGHEST, preferred_element_type=F32
    )
    partial = lax.dot_general(
        gradients, weight, NT, precision=lax.Precision.HIGHEST, preferred_element_type=F32
    )
    input_grad = lax.psum_scatter(partial, "dout", scatter_dimension=0, tiled=True)
    return (input_grad, weight_grad)


def halves(value):
    high = value.astype(BF16)
    low = (value - high.astype(F32)).astype(BF16)
    return high, low


def swap(value, axis, size, distance):
    return lax.ppermute(value, axis, [(i, i ^ distance) for i in range(size)])


def in_order(pieces, me):
    count = len(pieces)
    ordered = []
    for position in range(count):
        value = pieces[0][...]
        for s in range(1, count):
            value = jnp.where((me ^ s) == position, pieces[s][...], value)
        ordered.append(value)
    return ordered


def multiply(split_ref, rows, value):
    high, low = halves(value)
    both = lax.dot_general(split_ref[: 2 * rows], high, NT, preferred_element_type=F32)
    rest = lax.dot_general(split_ref[:rows], low, NT, preferred_element_type=F32)
    return both[:rows] + both[rows:] + rest


def aligned(index, tile):
    return pl.ds(pl.multiple_of(index * tile, tile), tile)


class Reader:
    def __init__(self, w_ref, slots, sems, first, steps):
        self.w, self.slots, self.sems = w_ref, slots, sems
        self.first, self.steps = first, steps
        self.ahead = min(slots.shape[0] - 1, steps)

    def copy(self, step):
        count, tile = self.slots.shape[:2]
        slot = lax.rem(step, count)
        return pltpu.make_async_copy(
            self.w.at[aligned(self.first + step, tile), :],
            self.slots.at[slot],
            self.sems.at[slot],
        )

    def begin(self):
        for step in range(self.ahead):
            self.copy(step).start()

    def arrive(self, step):
        self.copy(step).wait()

        @pl.when(step + self.ahead < self.steps)
        def _():
            self.copy(step + self.ahead).start()

    def take(self, step):
        return self.slots[lax.rem(step, self.slots.shape[0])]


class Writer:
    def __init__(self, left_ref, split_ref, out_ref, slots, sems, first, steps):
        self.left, self.split, self.out = left_ref, split_ref, out_ref
        self.slots, self.sems = slots, sems
        self.first, self.steps = first, steps
        self.cuts = sems.shape[1]

    def copies(self, step):
        count, tile, width = self.slots.shape
        slot = lax.rem(step, count)
        part = width // self.cuts
        return [
            pltpu.make_async_copy(
                self.slots.at[slot, :, pl.ds(k * part, part)],
                self.out.at[aligned(self.first + step, tile), pl.ds(k * part, part)],
                self.sems.at[slot, k],
            )
            for k in range(self.cuts)
        ]

    def make(self, step):
        count, tile, width = self.slots.shape
        part = width // self.cuts
        if count < self.steps:

            @pl.when(step >= count)
            def _():
                for copy in self.copies(step - count):
                    copy.wait()

        left = self.left[:, aligned(self.first + step, tile)]
        for k, copy in enumerate(self.copies(step)):
            self.slots[lax.rem(step, count), :, k * part : (k + 1) * part] = (
                lax.dot_general(
                    left,
                    self.split[:, k * part : (k + 1) * part],
                    TN,
                    preferred_element_type=F32,
                )
            )
            copy.start()

    def finish(self):
        for step in range(max(0, self.steps - self.slots.shape[0]), self.steps):
            for copy in self.copies(step):
                copy.wait()


def loop(steps, run):
    def one(step, carry):
        run(step)
        return carry

    lax.fori_loop(0, steps, one, 0)


def units_kernel(count, steps, *refs):
    grads, refs = refs[:count], refs[count:]
    w_ref, out_ref, split_ref, rows_ref, slots, sems = refs
    reader = Reader(w_ref, slots, sems, 0, steps)
    reader.begin()
    rows = rows_ref.shape[0]
    block = rows // count
    for position, value in enumerate(in_order(grads, lax.axis_index("din"))):
        rows_ref[position * block : (position + 1) * block, :] = value
    high, low = halves(rows_ref[...])
    split_ref[...] = jnp.concatenate([high, low, high], axis=0)

    def run(step):
        tile = slots.shape[1]
        reader.arrive(step)
        out_ref[:, aligned(step, tile)] = multiply(split_ref, rows, reader.take(step))

    loop(steps, run)


def in_vmem(count=1):
    return [pl.BlockSpec(memory_space=pltpu.VMEM)] * count


def in_hbm(count=1):
    return [pl.BlockSpec(memory_space=pltpu.MemorySpace.HBM)] * count


def ring(slots, tile, width, *cuts):
    return [
        pltpu.VMEM((slots, tile, width), F32),
        pltpu.SemaphoreType.DMA((slots, *cuts)),
    ]


def units(grads, weight, steps, tile):
    width = weight.shape[1]
    count = len(grads)
    rows = sum(piece.shape[0] for piece in grads)
    return pl.pallas_call(
        functools.partial(units_kernel, count, steps),
        out_shape=[
            pltpu.VMEM((rows, steps * tile), F32),
            pltpu.VMEM((3 * rows, width), BF16),
        ],
        in_specs=in_vmem(count) + in_hbm(),
        out_specs=in_vmem(2),
        scratch_shapes=[pltpu.VMEM((rows, width), F32)] + ring(READ_SLOTS, tile, width),
        compiler_params=pltpu.CompilerParams(vmem_limit_bytes=28 << 20),
        name="units",
    )(*grads, weight)


def outer_kernel(count, first, steps, *refs):
    pieces, refs = refs[:count], refs[count:]
    split_ref, left_ref, out_ref, slots, sems, *rows_ref = refs
    if count:
        rows = rows_ref[0].shape[0]
        block = rows // count
        for position, value in enumerate(in_order(pieces, lax.axis_index("dout") // 2)):
            rows_ref[0][position * block : (position + 1) * block, :] = value
        high, low = halves(rows_ref[0][...])
        left_ref[...] = jnp.concatenate([high, high, low], axis=0)
    writer = Writer(left_ref, split_ref, out_ref, slots, sems, first, steps)
    loop(steps, writer.make)
    writer.finish()


def later_kernel(first, steps, split_ref, left_ref, begun_ref, *refs):
    del begun_ref
    outer_kernel(0, first, steps, split_ref, left_ref, *refs)


def outer_first(pieces, split, steps, tile):
    depth, width = pieces[0].shape[1], split.shape[1]
    count = len(pieces)
    rows = split.shape[0] // 3
    return pl.pallas_call(
        functools.partial(outer_kernel, count, 0, steps),
        out_shape=[
            pltpu.VMEM((3 * rows, depth), BF16),
            jax.ShapeDtypeStruct((depth, width), F32),
        ],
        in_specs=in_vmem(count + 1),
        out_specs=in_vmem() + in_hbm(),
        scratch_shapes=ring(min(steps, WRITE_SLOTS), tile, width, CUTS)
        + [pltpu.VMEM((rows, depth), F32)],
        compiler_params=pltpu.CompilerParams(vmem_limit_bytes=24 << 20),
        name="outer_0",
    )(*pieces, split)


def outer(left, split, buffer, first, steps, tile):
    depth, width = left.shape[1], split.shape[1]
    return pl.pallas_call(
        functools.partial(later_kernel, first, steps),
        out_shape=jax.ShapeDtypeStruct((depth, width), F32),
        in_specs=in_vmem(2) + in_hbm(),
        out_specs=in_hbm()[0],
        scratch_shapes=ring(min(steps, WRITE_SLOTS), tile, width, CUTS),
        input_output_aliases={2: 0},
        compiler_params=pltpu.CompilerParams(vmem_limit_bytes=24 << 20),
    )(split, left, buffer)


def join_kernel(own_ref, other_ref, out_ref):
    half = own_ref.shape[0]
    upper = lax.axis_index("dout") % 2
    own, other = own_ref[...], other_ref[...]
    out_ref[:half, :] = jnp.where(upper == 1, other, own)
    out_ref[half:, :] = jnp.where(upper == 1, own, other)


def join(own, other, cost):
    rows, width = own.shape
    return pl.pallas_call(
        join_kernel,
        out_shape=jax.ShapeDtypeStruct((2 * rows, width), F32),
        in_specs=in_vmem(2),
        out_specs=in_vmem()[0],
        cost_estimate=pl.CostEstimate(
            flops=cost, bytes_accessed=0, transcendentals=0
        ),
        compiler_params=pltpu.CompilerParams(vmem_limit_bytes=2 << 20),
        name="join",
    )(own, other)


def bit_of(axis, distance):
    return (lax.axis_index(axis) // distance) % 2 == 1


def halved(value, n_out, distance):
    half = value.shape[0] // 2
    upper = bit_of("dout", distance)
    keep = jnp.where(upper, value[half:], value[:half])
    give = jnp.where(upper, value[:half], value[half:])
    return keep + swap(give, "dout", n_out, distance)


def body(n_in, n_out, inputs, out_grad, weight):
    depth = weight.shape[0]
    rounds = n_out.bit_length() - 1
    weight = pltpu.with_memory_space_constraint(weight, pltpu.MemorySpace.HBM)
    grads = [out_grad] + [swap(out_grad, "din", n_in, s) for s in range(1, n_in)]
    pair = join(inputs, swap(inputs, "dout", n_out, 1), 100000000000)
    pieces = [pair]
    pieces += [swap(pair, "dout", n_out, 2 * s) for s in range(1, n_out // 2)]
    total, split = units(grads, weight, depth // UNITS_TILE, UNITS_TILE)
    first, rest = 0, depth // OUTER_TILE
    for r in range(rounds):
        total = halved(total, n_out, n_out >> (r + 1))
        steps = (rest + rounds - 1 - r) // (rounds - r)
        rest -= steps
        if r == 0:
            left, weight_grad = outer_first(pieces, split, steps, OUTER_TILE)
        else:
            weight_grad = outer(left, split, weight_grad, first, steps, OUTER_TILE)
        first += steps
    return (total, weight_grad)


def power_of_two(value):
    return value & (value - 1) == 0


def solution(mesh):
    n_in, n_out = mesh.shape["din"], mesh.shape["dout"]
    shaped = (
        power_of_two(n_in) and power_of_two(n_out) and n_in <= 8 and 4 <= n_out <= 8
    )

    def run(inputs, out_grad, weight):
        depth, width = weight.shape
        fits = (
            inputs.shape[0] * n_out <= 64
            and depth % (2 * UNITS_TILE) == 0
            and depth >= 8 * UNITS_TILE
            and width % 128 == 0
        )
        if not (shaped and fits):
            return plain_body(inputs, out_grad, weight)
        return body(n_in, n_out, inputs, out_grad, weight)

    placed = (P("dout", "din"), P("din", "dout"), P("din", "dout"))
    return jax.shard_map(
        run,
        mesh=mesh,
        in_specs=placed,
        out_specs=(P("dout", "din"), P("din", "dout")),
        check_vma=False,
    )
```

```python
import functools

import jax
import jax.numpy as jnp
from jax import lax
from jax.experimental import pallas as pl
from jax.experimental.pallas import tpu as pltpu
from jax.sharding import PartitionSpec as P


F32 = jnp.float32
BF16 = jnp.bfloat16
TN = (((0,), (0,)), ((), ()))
NT = (((1,), (1,)), ((), ()))

UNITS_TILE = 256
OUTER_TILE = 128
READ_SLOTS = 4
WRITE_SLOTS = 4
CUTS = 2
MARK_FLOPS = 100_000_000_000


def plain_body(inputs, out_grad, weight):
    gradients = lax.all_gather(out_grad, "din", axis=0, tiled=True)
    rows = lax.all_gather(inputs, "dout", axis=0, tiled=True)
    weight_grad = lax.dot_general(
        rows, gradients, TN, precision=lax.Precision.HIGHEST, preferred_element_type=F32
    )
    partial = lax.dot_general(
        gradients, weight, NT, precision=lax.Precision.HIGHEST, preferred_element_type=F32
    )
    input_grad = lax.psum_scatter(partial, "dout", scatter_dimension=0, tiled=True)
    return (input_grad, weight_grad)


def halves(value):
    high = value.astype(BF16)
    low = (value - high.astype(F32)).astype(BF16)
    return high, low


def swap(value, axis, size, distance):
    return lax.ppermute(value, axis, [(i, i ^ distance) for i in range(size)])


def in_order(pieces, me):
    count = len(pieces)
    ordered = []
    for position in range(count):
        value = pieces[0][...]
        for s in range(1, count):
            value = jnp.where((me ^ s) == position, pieces[s][...], value)
        ordered.append(value)
    return ordered


def multiply(split_ref, rows, value):
    high, low = halves(value)
    both = lax.dot_general(split_ref[: 2 * rows], high, NT, preferred_element_type=F32)
    rest = lax.dot_general(split_ref[:rows], low, NT, preferred_element_type=F32)
    return both[:rows] + both[rows:] + rest


def aligned(index, tile):
    return pl.ds(pl.multiple_of(index * tile, tile), tile)


class Reader:
    def __init__(self, w_ref, slots, sems, first, steps):
        self.w, self.slots, self.sems = w_ref, slots, sems
        self.first, self.steps = first, steps
        self.ahead = min(slots.shape[0] - 1, steps)

    def copy(self, step):
        count, tile = self.slots.shape[:2]
        slot = lax.rem(step, count)
        return pltpu.make_async_copy(
            self.w.at[aligned(self.first + step, tile), :],
            self.slots.at[slot],
            self.sems.at[slot],
        )

    def begin(self):
        for step in range(self.ahead):
            self.copy(step).start()

    def arrive(self, step):
        self.copy(step).wait()

        @pl.when(step + self.ahead < self.steps)
        def _():
            self.copy(step + self.ahead).start()

    def take(self, step):
        return self.slots[lax.rem(step, self.slots.shape[0])]


class Writer:
    def __init__(self, left_ref, split_ref, out_ref, slots, sems, first, steps):
        self.left, self.split, self.out = left_ref, split_ref, out_ref
        self.slots, self.sems = slots, sems
        self.first, self.steps = first, steps
        self.cuts = sems.shape[1]

    def copies(self, step):
        count, tile, width = self.slots.shape
        slot = lax.rem(step, count)
        part = width // self.cuts
        return [
            pltpu.make_async_copy(
                self.slots.at[slot, :, pl.ds(k * part, part)],
                self.out.at[aligned(self.first + step, tile), pl.ds(k * part, part)],
                self.sems.at[slot, k],
            )
            for k in range(self.cuts)
        ]

    def make(self, step):
        count, tile, width = self.slots.shape
        part = width // self.cuts
        if count < self.steps:

            @pl.when(step >= count)
            def _():
                for copy in self.copies(step - count):
                    copy.wait()

        left = self.left[:, aligned(self.first + step, tile)]
        for k, copy in enumerate(self.copies(step)):
            self.slots[lax.rem(step, count), :, k * part : (k + 1) * part] = (
                lax.dot_general(
                    left,
                    self.split[:, k * part : (k + 1) * part],
                    TN,
                    preferred_element_type=F32,
                )
            )
            copy.start()

    def finish(self):
        for step in range(max(0, self.steps - self.slots.shape[0]), self.steps):
            for copy in self.copies(step):
                copy.wait()


def loop(steps, run):
    def one(step, carry):
        run(step)
        return carry

    lax.fori_loop(0, steps, one, 0)


def units_kernel(count, steps, *refs):
    grads, refs = refs[:count], refs[count:]
    w_ref, out_ref, split_ref, rows_ref, slots, sems = refs
    reader = Reader(w_ref, slots, sems, 0, steps)
    reader.begin()
    rows = rows_ref.shape[0]
    block = rows // count
    for position, value in enumerate(in_order(grads, lax.axis_index("din") // 2)):
        rows_ref[position * block : (position + 1) * block, :] = value
    high, low = halves(rows_ref[...])
    split_ref[...] = jnp.concatenate([high, low, high], axis=0)

    def run(step):
        tile = slots.shape[1]
        reader.arrive(step)
        out_ref[:, aligned(step, tile)] = multiply(split_ref, rows, reader.take(step))

    loop(steps, run)


def in_vmem(count=1):
    return [pl.BlockSpec(memory_space=pltpu.VMEM)] * count


def in_hbm(count=1):
    return [pl.BlockSpec(memory_space=pltpu.MemorySpace.HBM)] * count


def ring(slots, tile, width, *cuts):
    return [
        pltpu.VMEM((slots, tile, width), F32),
        pltpu.SemaphoreType.DMA((slots, *cuts)),
    ]


def units(grads, weight, steps, tile):
    width = weight.shape[1]
    count = len(grads)
    rows = sum(piece.shape[0] for piece in grads)
    return pl.pallas_call(
        functools.partial(units_kernel, count, steps),
        out_shape=[
            pltpu.VMEM((rows, steps * tile), F32),
            pltpu.VMEM((3 * rows, width), BF16),
        ],
        in_specs=in_vmem(count) + in_hbm(),
        out_specs=in_vmem(2),
        scratch_shapes=[pltpu.VMEM((rows, width), F32)] + ring(READ_SLOTS, tile, width),
        compiler_params=pltpu.CompilerParams(vmem_limit_bytes=28 << 20),
        name="units",
    )(*grads, weight)


def outer_kernel(count, first, steps, *refs):
    pieces, refs = refs[:count], refs[count:]
    split_ref, left_ref, out_ref, slots, sems, *rows_ref = refs
    if count:
        rows = rows_ref[0].shape[0]
        block = rows // count
        for position, value in enumerate(in_order(pieces, lax.axis_index("dout") // 2)):
            rows_ref[0][position * block : (position + 1) * block, :] = value
        high, low = halves(rows_ref[0][...])
        left_ref[...] = jnp.concatenate([high, high, low], axis=0)
    writer = Writer(left_ref, split_ref, out_ref, slots, sems, first, steps)
    loop(steps, writer.make)
    writer.finish()


def later_kernel(first, steps, split_ref, left_ref, begun_ref, *refs):
    del begun_ref
    outer_kernel(0, first, steps, split_ref, left_ref, *refs)


def outer_first(pieces, split, steps, tile):
    depth, width = pieces[0].shape[1], split.shape[1]
    count = len(pieces)
    rows = split.shape[0] // 3
    return pl.pallas_call(
        functools.partial(outer_kernel, count, 0, steps),
        out_shape=[
            pltpu.VMEM((3 * rows, depth), BF16),
            jax.ShapeDtypeStruct((depth, width), F32),
        ],
        in_specs=in_vmem(count + 1),
        out_specs=in_vmem() + in_hbm(),
        scratch_shapes=ring(min(steps, WRITE_SLOTS), tile, width, CUTS)
        + [pltpu.VMEM((rows, depth), F32)],
        compiler_params=pltpu.CompilerParams(vmem_limit_bytes=24 << 20),
        name="outer_0",
    )(*pieces, split)


def outer(left, split, buffer, first, steps, tile):
    depth, width = left.shape[1], split.shape[1]
    return pl.pallas_call(
        functools.partial(later_kernel, first, steps),
        out_shape=jax.ShapeDtypeStruct((depth, width), F32),
        in_specs=in_vmem(2) + in_hbm(),
        out_specs=in_hbm()[0],
        scratch_shapes=ring(min(steps, WRITE_SLOTS), tile, width, CUTS),
        input_output_aliases={2: 0},
        compiler_params=pltpu.CompilerParams(vmem_limit_bytes=24 << 20),
    )(split, left, buffer)


def mark_kernel(out_ref):
    out_ref[...] = jnp.zeros_like(out_ref)


def mark():
    return pl.pallas_call(
        mark_kernel,
        out_shape=pltpu.VMEM((8, 128), F32),
        out_specs=in_vmem()[0],
        cost_estimate=pl.CostEstimate(
            flops=MARK_FLOPS, bytes_accessed=0, transcendentals=0
        ),
        compiler_params=pltpu.CompilerParams(vmem_limit_bytes=2 << 20),
        name="mark",
    )()


def join_kernel(axis, own_ref, other_ref, point_ref, out_ref):
    del point_ref
    half = own_ref.shape[0]
    upper = lax.axis_index(axis) % 2
    own, other = own_ref[...], other_ref[...]
    out_ref[:half, :] = jnp.where(upper == 1, other, own)
    out_ref[half:, :] = jnp.where(upper == 1, own, other)


def join(own, axis, size, point):
    rows, width = own.shape
    return pl.pallas_call(
        functools.partial(join_kernel, axis),
        out_shape=jax.ShapeDtypeStruct((2 * rows, width), F32),
        in_specs=in_vmem(3),
        out_specs=in_vmem()[0],
        compiler_params=pltpu.CompilerParams(vmem_limit_bytes=4 << 20),
    )(own, swap(own, axis, size, 1), point)


def spread(pair, axis, size):
    return [pair] + [swap(pair, axis, size, 2 * s) for s in range(1, size // 2)]


def bit_of(axis, distance):
    return (lax.axis_index(axis) // distance) % 2 == 1


def halved(value, n_out, distance):
    half = value.shape[0] // 2
    upper = bit_of("dout", distance)
    keep = jnp.where(upper, value[half:], value[:half])
    give = jnp.where(upper, value[:half], value[half:])
    return keep + swap(give, "dout", n_out, distance)


def body(n_in, n_out, inputs, out_grad, weight):
    depth = weight.shape[0]
    rounds = n_out.bit_length() - 1
    weight = pltpu.with_memory_space_constraint(weight, pltpu.MemorySpace.HBM)
    point = mark()
    pair = join(out_grad, "din", n_in, point)
    grads = spread(pair, "din", n_in)
    pair = join(inputs, "dout", n_out, point)
    pieces = spread(pair, "dout", n_out)
    total, split = units(grads, weight, depth // UNITS_TILE, UNITS_TILE)
    first, rest = 0, depth // OUTER_TILE
    for r in range(rounds):
        total = halved(total, n_out, n_out >> (r + 1))
        steps = (rest + rounds - 1 - r) // (rounds - r)
        rest -= steps
        if r == 0:
            left, weight_grad = outer_first(pieces, split, steps, OUTER_TILE)
        else:
            weight_grad = outer(left, split, weight_grad, first, steps, OUTER_TILE)
        first += steps
    return (total, weight_grad)


def power_of_two(value):
    return value & (value - 1) == 0


def solution(mesh):
    n_in, n_out = mesh.shape["din"], mesh.shape["dout"]
    shaped = (
        power_of_two(n_in) and power_of_two(n_out) and 4 <= n_in <= 8 and 4 <= n_out <= 8
    )

    def run(inputs, out_grad, weight):
        depth, width = weight.shape
        fits = (
            inputs.shape[0] * n_out <= 64
            and depth % (2 * UNITS_TILE) == 0
            and depth >= 8 * UNITS_TILE
            and width % 128 == 0
        )
        if not (shaped and fits):
            return plain_body(inputs, out_grad, weight)
        return body(n_in, n_out, inputs, out_grad, weight)

    placed = (P("dout", "din"), P("din", "dout"), P("din", "dout"))
    return jax.shard_map(
        run,
        mesh=mesh,
        in_specs=placed,
        out_specs=(P("dout", "din"), P("din", "dout")),
        check_vma=False,
    )
```

```python
import functools

import jax
import jax.numpy as jnp
from jax import lax
from jax.experimental import pallas as pl
from jax.experimental.pallas import tpu as pltpu
from jax.sharding import PartitionSpec as P


F32 = jnp.float32
BF16 = jnp.bfloat16
TN = (((0,), (0,)), ((), ()))
NT = (((1,), (1,)), ((), ()))

UNITS_TILE = 256
OUTER_TILE = 128
READ_SLOTS = 6
WRITE_SLOTS = 4
CUTS = 2
MARK_FLOPS = 100_000_000_000


def plain_body(inputs, out_grad, weight):
    gradients = lax.all_gather(out_grad, "din", axis=0, tiled=True)
    rows = lax.all_gather(inputs, "dout", axis=0, tiled=True)
    weight_grad = lax.dot_general(
        rows, gradients, TN, precision=lax.Precision.HIGHEST, preferred_element_type=F32
    )
    partial = lax.dot_general(
        gradients, weight, NT, precision=lax.Precision.HIGHEST, preferred_element_type=F32
    )
    input_grad = lax.psum_scatter(partial, "dout", scatter_dimension=0, tiled=True)
    return (input_grad, weight_grad)


def halves(value):
    high = value.astype(BF16)
    low = (value - high.astype(F32)).astype(BF16)
    return high, low


def swap(value, axis, size, distance):
    return lax.ppermute(value, axis, [(i, i ^ distance) for i in range(size)])


def in_order(pieces, me):
    count = len(pieces)
    ordered = []
    for position in range(count):
        value = pieces[0][...]
        for s in range(1, count):
            value = jnp.where((me ^ s) == position, pieces[s][...], value)
        ordered.append(value)
    return ordered


def multiply(split_ref, rows, value):
    high, low = halves(value)
    both = lax.dot_general(split_ref[: 2 * rows], high, NT, preferred_element_type=F32)
    rest = lax.dot_general(split_ref[:rows], low, NT, preferred_element_type=F32)
    return both[:rows] + both[rows:] + rest


def aligned(index, tile):
    return pl.ds(pl.multiple_of(index * tile, tile), tile)


class Reader:
    def __init__(self, w_ref, slots, sems, first, steps):
        self.w, self.slots, self.sems = w_ref, slots, sems
        self.first, self.steps = first, steps
        self.ahead = min(slots.shape[0] - 1, steps)

    def copy(self, step):
        count, tile = self.slots.shape[:2]
        slot = lax.rem(step, count)
        return pltpu.make_async_copy(
            self.w.at[aligned(self.first + step, tile), :],
            self.slots.at[slot],
            self.sems.at[slot],
        )

    def begin(self, first, last):
        for step in range(first, min(last, self.ahead)):
            self.copy(step).start()

    def arrive(self, step):
        self.copy(step).wait()

        @pl.when(step + self.ahead < self.steps)
        def _():
            self.copy(step + self.ahead).start()

    def take(self, step):
        return self.slots[lax.rem(step, self.slots.shape[0])]


class Writer:
    def __init__(self, left_ref, split_ref, out_ref, slots, sems, first, steps):
        self.left, self.split, self.out = left_ref, split_ref, out_ref
        self.slots, self.sems = slots, sems
        self.first, self.steps = first, steps
        self.cuts = sems.shape[1]

    def copies(self, step):
        count, tile, width = self.slots.shape
        slot = lax.rem(step, count)
        part = width // self.cuts
        return [
            pltpu.make_async_copy(
                self.slots.at[slot, :, pl.ds(k * part, part)],
                self.out.at[aligned(self.first + step, tile), pl.ds(k * part, part)],
                self.sems.at[slot, k],
            )
            for k in range(self.cuts)
        ]

    def make(self, step):
        count, tile, width = self.slots.shape
        part = width // self.cuts
        if count < self.steps:

            @pl.when(step >= count)
            def _():
                for copy in self.copies(step - count):
                    copy.wait()

        left = self.left[:, aligned(self.first + step, tile)]
        for k, copy in enumerate(self.copies(step)):
            self.slots[lax.rem(step, count), :, k * part : (k + 1) * part] = (
                lax.dot_general(
                    left,
                    self.split[:, k * part : (k + 1) * part],
                    TN,
                    preferred_element_type=F32,
                )
            )
            copy.start()

    def finish(self):
        for step in range(max(0, self.steps - self.slots.shape[0]), self.steps):
            for copy in self.copies(step):
                copy.wait()


def loop(steps, run):
    def one(step, carry):
        run(step)
        return carry

    lax.fori_loop(0, steps, one, 0)


def units_kernel(count, steps, *refs):
    grads, refs = refs[:count], refs[count:]
    w_ref, out_ref, split_ref, rows_ref, slots, sems = refs
    reader = Reader(w_ref, slots, sems, 0, steps)
    reader.begin(0, 1)
    rows = rows_ref.shape[0]
    block = rows // count
    for position, value in enumerate(in_order(grads, lax.axis_index("din") // 2)):
        rows_ref[position * block : (position + 1) * block, :] = value
    high, low = halves(rows_ref[...])
    split_ref[...] = jnp.concatenate([high, low, high], axis=0)
    reader.begin(1, READ_SLOTS)

    def run(step):
        tile = slots.shape[1]
        reader.arrive(step)
        out_ref[:, aligned(step, tile)] = multiply(split_ref, rows, reader.take(step))

    loop(steps, run)


def in_vmem(count=1):
    return [pl.BlockSpec(memory_space=pltpu.VMEM)] * count


def in_hbm(count=1):
    return [pl.BlockSpec(memory_space=pltpu.MemorySpace.HBM)] * count


def ring(slots, tile, width, *cuts):
    return [
        pltpu.VMEM((slots, tile, width), F32),
        pltpu.SemaphoreType.DMA((slots, *cuts)),
    ]


def units(grads, weight, steps, tile):
    width = weight.shape[1]
    count = len(grads)
    rows = sum(piece.shape[0] for piece in grads)
    return pl.pallas_call(
        functools.partial(units_kernel, count, steps),
        out_shape=[
            pltpu.VMEM((rows, steps * tile), F32),
            pltpu.VMEM((3 * rows, width), BF16),
        ],
        in_specs=in_vmem(count) + in_hbm(),
        out_specs=in_vmem(2),
        scratch_shapes=[pltpu.VMEM((rows, width), F32)] + ring(READ_SLOTS, tile, width),
        compiler_params=pltpu.CompilerParams(vmem_limit_bytes=28 << 20),
        name="units",
    )(*grads, weight)


def outer_kernel(count, first, steps, *refs):
    pieces, refs = refs[:count], refs[count:]
    split_ref, left_ref, out_ref, slots, sems, *rows_ref = refs
    if count:
        rows = rows_ref[0].shape[0]
        block = rows // count
        for position, value in enumerate(in_order(pieces, lax.axis_index("dout") // 2)):
            rows_ref[0][position * block : (position + 1) * block, :] = value
        high, low = halves(rows_ref[0][...])
        left_ref[...] = jnp.concatenate([high, high, low], axis=0)
    writer = Writer(left_ref, split_ref, out_ref, slots, sems, first, steps)
    loop(steps, writer.make)
    writer.finish()


def later_kernel(first, steps, split_ref, left_ref, begun_ref, *refs):
    del begun_ref
    outer_kernel(0, first, steps, split_ref, left_ref, *refs)


def outer_first(pieces, split, steps, tile):
    depth, width = pieces[0].shape[1], split.shape[1]
    count = len(pieces)
    rows = split.shape[0] // 3
    return pl.pallas_call(
        functools.partial(outer_kernel, count, 0, steps),
        out_shape=[
            pltpu.VMEM((3 * rows, depth), BF16),
            jax.ShapeDtypeStruct((depth, width), F32),
        ],
        in_specs=in_vmem(count + 1),
        out_specs=in_vmem() + in_hbm(),
        scratch_shapes=ring(min(steps, WRITE_SLOTS), tile, width, CUTS)
        + [pltpu.VMEM((rows, depth), F32)],
        compiler_params=pltpu.CompilerParams(vmem_limit_bytes=24 << 20),
        name="outer_0",
    )(*pieces, split)


def outer(left, split, buffer, first, steps, tile):
    depth, width = left.shape[1], split.shape[1]
    return pl.pallas_call(
        functools.partial(later_kernel, first, steps),
        out_shape=jax.ShapeDtypeStruct((depth, width), F32),
        in_specs=in_vmem(2) + in_hbm(),
        out_specs=in_hbm()[0],
        scratch_shapes=ring(min(steps, WRITE_SLOTS), tile, width, CUTS),
        input_output_aliases={2: 0},
        compiler_params=pltpu.CompilerParams(vmem_limit_bytes=24 << 20),
    )(split, left, buffer)


def mark_kernel(out_ref):
    out_ref[...] = jnp.zeros_like(out_ref)


def mark():
    return pl.pallas_call(
        mark_kernel,
        out_shape=pltpu.VMEM((8, 128), F32),
        out_specs=in_vmem()[0],
        cost_estimate=pl.CostEstimate(
            flops=MARK_FLOPS, bytes_accessed=0, transcendentals=0
        ),
        compiler_params=pltpu.CompilerParams(vmem_limit_bytes=2 << 20),
        name="mark",
    )()


def join_kernel(axis, own_ref, other_ref, point_ref, out_ref):
    del point_ref
    half = own_ref.shape[0]
    upper = lax.axis_index(axis) % 2
    own, other = own_ref[...], other_ref[...]
    out_ref[:half, :] = jnp.where(upper == 1, other, own)
    out_ref[half:, :] = jnp.where(upper == 1, own, other)


def join(own, axis, size, point):
    rows, width = own.shape
    return pl.pallas_call(
        functools.partial(join_kernel, axis),
        out_shape=jax.ShapeDtypeStruct((2 * rows, width), F32),
        in_specs=in_vmem(3),
        out_specs=in_vmem()[0],
        compiler_params=pltpu.CompilerParams(vmem_limit_bytes=4 << 20),
    )(own, swap(own, axis, size, 1), point)


def spread(pair, axis, size):
    return [pair] + [swap(pair, axis, size, 2 * s) for s in range(1, size // 2)]


def bit_of(axis, distance):
    return (lax.axis_index(axis) // distance) % 2 == 1


def halved(value, n_out, distance):
    half = value.shape[0] // 2
    upper = bit_of("dout", distance)
    keep = jnp.where(upper, value[half:], value[:half])
    give = jnp.where(upper, value[:half], value[half:])
    return keep + swap(give, "dout", n_out, distance)


def body(n_in, n_out, inputs, out_grad, weight):
    depth = weight.shape[0]
    rounds = n_out.bit_length() - 1
    weight = pltpu.with_memory_space_constraint(weight, pltpu.MemorySpace.HBM)
    point = mark()
    pair = join(out_grad, "din", n_in, point)
    grads = spread(pair, "din", n_in)
    pair = join(inputs, "dout", n_out, point)
    pieces = spread(pair, "dout", n_out)
    total, split = units(grads, weight, depth // UNITS_TILE, UNITS_TILE)
    first, rest = 0, depth // OUTER_TILE
    for r in range(rounds):
        total = halved(total, n_out, n_out >> (r + 1))
        steps = (rest + rounds - 1 - r) // (rounds - r)
        rest -= steps
        if r == 0:
            left, weight_grad = outer_first(pieces, split, steps, OUTER_TILE)
        else:
            weight_grad = outer(left, split, weight_grad, first, steps, OUTER_TILE)
        first += steps
    return (total, weight_grad)


def power_of_two(value):
    return value & (value - 1) == 0


def solution(mesh):
    n_in, n_out = mesh.shape["din"], mesh.shape["dout"]
    shaped = (
        power_of_two(n_in) and power_of_two(n_out) and 4 <= n_in <= 8 and 4 <= n_out <= 8
    )

    def run(inputs, out_grad, weight):
        depth, width = weight.shape
        fits = (
            inputs.shape[0] * n_out <= 64
            and depth % (2 * UNITS_TILE) == 0
            and depth >= 8 * UNITS_TILE
            and width % 128 == 0
        )
        if not (shaped and fits):
            return plain_body(inputs, out_grad, weight)
        return body(n_in, n_out, inputs, out_grad, weight)

    placed = (P("dout", "din"), P("din", "dout"), P("din", "dout"))
    return jax.shard_map(
        run,
        mesh=mesh,
        in_specs=placed,
        out_specs=(P("dout", "din"), P("din", "dout")),
        check_vma=False,
    )
```
